256 devices in a mesh: rows: 64 (over y, z, core), grp: 4 (over x).
Axes of the slice: x: 4, y: 4, z: 8, core: 2. Of those that a mesh axis runs over, the one named last changes fastest.
Arguments:
- panel: float32 [65536, 256], P(('rows', 'grp')), may hold values from -6000 to 6000
- trailing: float32 [65536, 2048], P(('rows', 'grp')), may hold values from -6000 to 6000
Outputs:
- upper_panel: float32 [256, 256], replicated
- projection: float32 [256, 2048], replicated
- updated: float32 [65536, 2048], P(('rows', 'grp'))
- upper_next: float32 [256, 256], replicated
The draws below stay inside these ranges and needn't reach their ends.
All inputs are finite; a program needn't handle non-finite values.
Results may differ from the reference program's by a relative error of at most 0.00019.
Values sent between devices are 32-bit elements; how exact they have to be, the bound alone decides.
A program may use at most 128 MiB of HBM per device.

```python
import math
import jax
import jax.numpy as jnp
from jax import lax

PB = 256
TC = 2048
NROWS = 65536


def row_scale(key):
    position = jnp.arange(NROWS, dtype=jnp.float32) / max(NROWS - 1, 1)
    jitter = jnp.exp(jax.random.uniform(jax.random.fold_in(key, 11), (NROWS, 1), jnp.float32, 0.0, math.log(10.0)))
    return (3.0 ** position)[:, None] * jitter


def mixed_block(key, salt):
    coupling = jax.random.normal(jax.random.fold_in(key, salt), (PB, PB), jnp.float32)
    return jnp.eye(PB, dtype=jnp.float32) + 0.25 * coupling / math.sqrt(PB)


def panel_values(key):
    normals = jax.random.normal(jax.random.fold_in(key, 1), (NROWS, PB), jnp.float32)
    values = jnp.dot(normals, mixed_block(key, 2), precision=lax.Precision.HIGHEST)
    spread = math.log(10.0)
    column_scale = jnp.exp(jax.random.uniform(jax.random.fold_in(key, 3), (PB,), jnp.float32, 0.0, spread))
    return values * column_scale * row_scale(key)


def draw_panel(key, part):
    return panel_values(key)


def draw_trailing(key, part):
    values = panel_values(key)
    loading = jax.random.normal(jax.random.fold_in(key, 5), (PB, TC), jnp.float32) / math.sqrt(PB)
    normals = jax.random.normal(jax.random.fold_in(key, 6), (NROWS, TC), jnp.float32)
    leading = jnp.dot(normals[:, :PB], mixed_block(key, 7), precision=lax.Precision.HIGHEST)
    noise_part = jnp.concatenate([leading, normals[:, PB:]], axis=1)
    spread = math.log(10.0)
    column_scale = jnp.exp(jax.random.uniform(jax.random.fold_in(key, 8), (TC,), jnp.float32, 0.0, spread))
    noise_part = noise_part * column_scale * row_scale(key)
    return jnp.dot(values, loading, precision=lax.Precision.HIGHEST) + noise_part


def setup_inputs(seed: int = 0) -> dict:
    splits = jax.random.split(jax.random.key(seed), 3)
    panel = draw_panel(jax.random.fold_in(splits[2], 71), 0)
    trailing = draw_trailing(jax.random.fold_in(splits[2], 71), 0)
    return {"panel": panel, "trailing": trailing}


def cross(left, right):
    return lax.dot_general(left.astype(jnp.float32), right.astype(jnp.float32), (((0,), (0,)), ((), ())), precision=lax.Precision.HIGHEST, preferred_element_type=jnp.float32)

def upper_of(matrix):
    return jnp.linalg.cholesky(matrix).T

def reference(panel, trailing):
    inv_rows = 1.0 / panel.shape[0]
    width = panel.shape[1]
    upper_panel = upper_of(cross(panel, panel) * inv_rows)
    inverse = lax.linalg.triangular_solve(upper_panel, jnp.eye(width, dtype=upper_panel.dtype), left_side=True, lower=False)
    ortho_basis = jnp.dot(panel.astype(jnp.float32), inverse.astype(jnp.float32), precision=lax.Precision.HIGHEST, preferred_element_type=jnp.float32)
    projection = cross(ortho_basis, trailing) * inv_rows
    updated = trailing - jnp.dot(ortho_basis.astype(jnp.float32), projection.astype(jnp.float32), precision=lax.Precision.HIGHEST, preferred_element_type=jnp.float32)
    leading = updated[:, :width]
    upper_next = upper_of(cross(leading, leading) * inv_rows)
    return (upper_panel, projection, updated, upper_next)
```

```python
import jax
import jax.numpy as jnp
from jax import lax
from jax.experimental import pallas as pl
from jax.experimental.pallas import tpu as pltpu
from jax.sharding import PartitionSpec as P

PB = 256
TC = 2048
WIDE = TC + 2 * PB
HALF = 128
SUB = 8
NX, NY, NZ = 4, 4, 8
INV_ROWS = 1.0 / 65536
VMEM = pl.BlockSpec(memory_space=pltpu.VMEM)


def dot(left, right, dims=(1, 0)):
    return lax.dot_general(
        left,
        right,
        (((dims[0],), (dims[1],)), ((), ())),
        precision=lax.Precision.HIGHEST,
        preferred_element_type=jnp.float32,
    )


def identity(order):
    rows = lax.broadcasted_iota(jnp.int32, (order, order), 0)
    columns = lax.broadcasted_iota(jnp.int32, (order, order), 1)
    return (rows == columns).astype(jnp.float32)


def aligned(value, step):
    return pl.multiple_of(value, step)


class Stream:
    def __init__(self, place, acc, out, first, width, x_first, split_z, bufs, send, recv):
        self.acc, self.out = acc, out
        self.columns = pl.ds(first, width)
        self.first, self.width, self.split_z = first, width, split_z
        self.core_buf, self.major_buf, self.minor_buf, self.z_buf = bufs
        self.send, self.recv = send, recv
        self.place = place
        x, y, z, core = place
        self.x_first = x_first
        self.major, self.minor = (x, y) if x_first else (y, x)
        self.base = core * 128
        self.slab = self.base + self.major * 32
        self.own = self.slab + self.minor * 8

    def device(self, axis, value):
        x, y, z, core = self.place
        if axis == "major":
            axis = "x" if self.x_first else "y"
        elif axis == "minor":
            axis = "y" if self.x_first else "x"
        if axis == "x":
            x = value
        elif axis == "y":
            y = value
        elif axis == "z":
            z = value
        else:
            core = value
        return ((y * NZ + z) * 2 + core, x)

    def rows(self, start, size):
        return pl.ds(aligned(start, 8), size)

    def piece(self, z):
        part = self.width // NZ
        return pl.ds(aligned(self.first + z * part, 128), part)

    def phase(self, name):
        acc, out, columns, z = self.acc, self.out, self.columns, self.place[2]
        other = 1 - self.place[3]
        if name == "core":
            return [(acc.at[self.rows(other * 128, 128), columns], self.core_buf, "core", other)]
        if name == "core_share":
            here = out.at[self.rows(self.base, 128), columns]
            return [(here, here, "core", other)]
        copies = []
        for d in range(1, NZ if name in ("z", "z_share") else 4):
            if name == "major":
                peer = lax.rem(self.major + d, 4)
                src = acc.at[self.rows(self.base + peer * 32, 32), columns]
                copies.append((src, self.major_buf.at[d - 1], "major", peer))
            elif name == "minor":
                peer = lax.rem(self.minor + d, 4)
                src = acc.at[self.rows(self.slab + peer * 8, 8), columns]
                copies.append((src, self.minor_buf.at[d - 1], "minor", peer))
            elif name == "z":
                peer = lax.rem(z + d, NZ)
                src = acc.at[self.rows(self.own, 8), self.piece(peer) if self.split_z else columns]
                copies.append((src, self.z_buf.at[d - 1], "z", peer))
            elif name == "z_share":
                here = out.at[self.rows(self.own, 8), self.piece(z)]
                copies.append((here, here, "z", lax.rem(z + d, NZ)))
            elif name == "minor_share":
                here = out.at[self.rows(self.own, 8), columns]
                copies.append((here, here, "minor", lax.rem(self.minor + d, 4)))
            else:
                here = out.at[self.rows(self.slab, 32), columns]
                copies.append((here, here, "major", lax.rem(self.major + d, 4)))
        return copies

    def copies(self, name):
        return [
            pltpu.make_async_remote_copy(
                src_ref=src,
                dst_ref=dst,
                send_sem=self.send.at[FIRST[name] + index],
                recv_sem=self.recv.at[FIRST[name] + index],
                device_id=self.device(axis, peer),
                device_id_type=pl.DeviceIdType.MESH,
            )
            for index, (src, dst, axis, peer) in enumerate(self.phase(name))
        ]

    def start(self, name):
        if name == "z_share" and not self.split_z:
            return
        for copy in self.copies(name):
            copy.start()

    def wait(self, name):
        if name == "z_share" and not self.split_z:
            return
        for copy in self.copies(name):
            copy.wait()

    def core_end(self):
        self.wait("core")

        @pl.loop(0, 16)
        def _(step):
            here = self.rows(self.base + step * 8, 8)
            there = pl.ds(aligned(step * 8, 8), 8)
            self.acc[here, self.columns] = self.acc[here, self.columns] + self.core_buf[there, :]

    def major_end(self):
        self.wait("major")

        @pl.loop(0, 4)
        def _(step):
            here = self.rows(self.slab + step * 8, 8)
            there = pl.ds(aligned(step * 8, 8), 8)
            total = self.acc[here, self.columns]
            for d in range(3):
                total = total + self.major_buf[d, there, :]
            self.acc[here, self.columns] = total

    def minor_end(self):
        self.wait("minor")
        here = self.rows(self.own, 8)
        total = self.acc[here, self.columns]
        for d in range(3):
            total = total + self.minor_buf[d]
        self.acc[here, self.columns] = total

    def z_end(self):
        self.wait("z")
        here = self.rows(self.own, 8)
        columns = self.piece(self.place[2]) if self.split_z else self.columns
        total = self.acc[here, columns]
        for d in range(NZ - 1):
            total = total + self.z_buf[d]
        self.out[here, columns] = total

    def turn(self, before, after):
        self.wait(before)
        self.start(after)


FIRST = {
    "core": 0,
    "major": 1,
    "minor": 4,
    "z": 7,
    "z_share": 14,
    "minor_share": 21,
    "major_share": 24,
    "core_share": 27,
}
COPIES = 28

CROSS = 2 * PB
STREAMS = ((0, 256, True, False), (256, 512, True, False), (768, 1024, True, True), (1792, 768, False, False))


def greet(place):
    x, y, z, core = place
    peers = [((y * NZ + z) * 2 + 1 - core, x)]
    peers += [((y * NZ + z) * 2 + core, lax.rem(x + d, NX)) for d in range(1, NX)]
    peers += [((lax.rem(y + d, NY) * NZ + z) * 2 + core, x) for d in range(1, NY)]
    peers += [((y * NZ + lax.rem(z + d, NZ)) * 2 + core, x) for d in range(1, NZ)]
    barrier = pltpu.get_barrier_semaphore()
    for peer in peers:
        pl.semaphore_signal(barrier, inc=1, device_id=peer, device_id_type=pl.DeviceIdType.MESH)
    return barrier, len(peers)


def factor_half(work, upper, inverse, between):
    full = (SUB, HALF)
    lane = lax.broadcasted_iota(jnp.int32, (1, HALF), 1)
    for block in range(HALF // SUB):
        between(block)
        base = block * SUB
        left = [jnp.broadcast_to(work[base + i : base + i + 1, :HALF], full) for i in range(SUB)]
        right = [jnp.broadcast_to(work[base + i : base + i + 1, HALF:], full) for i in range(SUB)]
        entry = [
            [jnp.broadcast_to(left[i][:, base + k : base + k + 1], full) for k in range(i + 1)]
            for i in range(SUB)
        ]
        unit = [[None] * SUB for _ in range(SUB)]
        recip = [None] * SUB
        for k in range(SUB):
            recip[k] = 1.0 / entry[k][k]
            for j in range(k + 1, SUB):
                unit[j][k] = entry[j][k] * recip[k]
            for j in range(k + 1, SUB):
                for i in range(j, SUB):
                    entry[i][j] = entry[i][j] - entry[i][k] * unit[j][k]
                left[j] = left[j] - unit[j][k] * left[k]
                right[j] = right[j] - unit[j][k] * right[k]
        for k in range(SUB):
            scale = lax.rsqrt(entry[k][k])
            row = base + k
            upper[row : row + 1, :] = jnp.where(lane >= row, (left[k] * scale)[0:1, :], 0.0)
            inverse[row : row + 1, :] = (right[k] * scale)[0:1, :]
        if base + SUB == HALF:
            break
        for k in range(SUB - 1, -1, -1):
            left[k] = left[k] * recip[k]
            right[k] = right[k] * recip[k]
            for j in range(k + 1, SUB):
                left[k] = left[k] - unit[j][k] * left[j]
                right[k] = right[k] - unit[j][k] * right[j]
        for other in range(base + SUB, HALF, SUB):
            rows = slice(other, other + SUB)
            lead = work[rows, :HALF]
            tail = work[rows, HALF:]
            column = [jnp.broadcast_to(lead[:, base + k : base + k + 1], full) for k in range(SUB)]
            for k in range(SUB):
                lead = lead - column[k] * left[k]
                tail = tail - column[k] * right[k]
            work[rows, :HALF] = lead
            work[rows, HALF:] = tail


def reduce_kernel(panel, trailing, out, upper, inverse, upper_next, acc, work, halves, inverses, middle, schur, *scratch):
    row = lax.axis_index("rows")
    x = lax.axis_index("grp")
    core = lax.rem(row, 2)
    z = lax.rem(row // 2, NZ)
    y = row // (2 * NZ)
    place = (x, y, z, core)
    barrier, greeted = greet(place)

    streams = []
    for index, (first, width, x_first, split_z) in enumerate(STREAMS):
        bufs, send, recv = scratch[6 * index : 6 * index + 4], *scratch[6 * index + 4 : 6 * index + 6]
        streams.append(Stream(place, acc, out, first, width, x_first, split_z, bufs, send, recv))
    gram, head, one, two = streams

    def products(first, last):
        @pl.loop(first, last)
        def _(tile):
            columns = pl.ds(aligned(tile * PB, PB), PB)
            acc[:, pl.ds(aligned(CROSS + tile * PB, PB), PB)] = dot(panel[...], trailing[:, columns], (0, 0))

    acc[:, :PB] = dot(panel[...], panel[...], (0, 0))
    pl.semaphore_wait(barrier, greeted)
    gram.start("core")
    acc[:, PB : 2 * PB] = dot(trailing[:, :PB], trailing[:, :PB], (0, 0))
    gram.core_end()
    gram.start("major")
    acc[:, CROSS : CROSS + PB] = dot(panel[...], trailing[:, :PB], (0, 0))
    head.start("core")
    products(1, 5)
    head.core_end()
    one.start("core")
    gram.major_end()
    gram.start("minor")
    head.start("major")
    products(5, TC // PB)
    two.start("core")
    gram.minor_end()
    gram.start("z")
    one.core_end()
    head.major_end()
    head.start("minor")
    one.start("major")
    two.core_end()
    gram.z_end()
    gram.start("minor_share")
    head.minor_end()
    head.start("z")
    gram.turn("minor_share", "major_share")
    two.start("major")
    gram.turn("major_share", "core_share")
    head.z_end()
    head.start("minor_share")
    gram.wait("core_share")

    def meet_first():
        head.turn("minor_share", "major_share")
        one.major_end()
        one.start("minor")

    def meet_second():
        head.turn("major_share", "core_share")
        two.major_end()
        two.start("minor")

    def meet_third():
        one.minor_end()
        one.start("z")

    def meet_fourth():
        two.minor_end()
        two.start("z")

    def meet_fifth():
        one.z_end()
        one.start("z_share")
        two.z_end()
        two.start("minor_share")

    def meet_sixth():
        head.wait("core_share")
        one.turn("z_share", "minor_share")
        two.turn("minor_share", "major_share")

    def meet_seventh():
        one.turn("minor_share", "major_share")

    def meet_eighth():
        two.turn("major_share", "core_share")

    def meet_last():
        one.turn("major_share", "core_share")

    meetings = (
        (0, 2, meet_first),
        (0, 10, meet_second),
        (0, 14, meet_third),
        (1, 2, meet_fourth),
        (1, 9, meet_fifth),
        (1, 15, meet_sixth),
        (2, 10, meet_seventh),
        (3, 2, meet_eighth),
        (3, 12, meet_last),
    )

    zeros = jnp.zeros((HALF, HALF), jnp.float32)
    work[:, :HALF] = out[:HALF, :HALF] * INV_ROWS
    work[:, HALF:] = identity(HALF)
    schur[...] = out[:, :PB] * INV_ROWS

    @pl.loop(0, 4)
    def _(step):
        @pl.when(lax.rem(step, 2) == 1)
        def _():
            cross = dot(inverses[0], schur[:HALF, HALF:])
            middle[...] = cross
            work[:, :HALF] = schur[HALF:, HALF:] - dot(cross, cross, (0, 0))
            work[:, HALF:] = identity(HALF)

        @pl.when(step == 2)
        def _():
            upper[:HALF, :HALF] = halves[0]
            upper[:HALF, HALF:] = middle[...]
            upper[HALF:, :HALF] = zeros
            upper[HALF:, HALF:] = halves[1]
            inverse[:HALF, :HALF] = inverses[0]
            inverse[:HALF, HALF:] = zeros
            inverse[HALF:, :HALF] = -dot(inverses[1], dot(middle[...], inverses[0], (0, 0)))
            inverse[HALF:, HALF:] = inverses[1]
            part = dot(inverse[...], out[:, CROSS : CROSS + PB] * INV_ROWS)
            schur[...] = out[:, PB : 2 * PB] * INV_ROWS - dot(part, part, (0, 0))
            work[:, :HALF] = schur[:HALF, :HALF]
            work[:, HALF:] = identity(HALF)

        def between(block):
            for at_step, at_block, action in meetings:
                if at_block == block:
                    pl.when(step == at_step)(action)

        at = lax.rem(step, 2)
        factor_half(work, halves.at[at], inverses.at[at], between)

    upper_next[:HALF, :HALF] = halves[0]
    upper_next[:HALF, HALF:] = middle[...]
    upper_next[HALF:, :HALF] = zeros
    upper_next[HALF:, HALF:] = halves[1]
    one.wait("core_share")
    two.wait("core_share")


def reduced(panel, trailing):
    square = jax.ShapeDtypeStruct((PB, PB), jnp.float32)
    scratch = [
        pltpu.VMEM((PB, WIDE), jnp.float32),
        pltpu.VMEM((HALF, PB), jnp.float32),
        pltpu.VMEM((2, HALF, HALF), jnp.float32),
        pltpu.VMEM((2, HALF, HALF), jnp.float32),
        pltpu.VMEM((HALF, HALF), jnp.float32),
        pltpu.VMEM((PB, PB), jnp.float32),
    ]
    for _, width, _, split_z in STREAMS:
        part = width // NZ if split_z else width
        scratch += [
            pltpu.VMEM((128, width), jnp.float32),
            pltpu.VMEM((3, 32, width), jnp.float32),
            pltpu.VMEM((3, 8, width), jnp.float32),
            pltpu.VMEM((NZ - 1, 8, part), jnp.float32),
            pltpu.SemaphoreType.DMA((COPIES,)),
            pltpu.SemaphoreType.DMA((COPIES,)),
        ]
    return pl.pallas_call(
        reduce_kernel,
        out_shape=(jax.ShapeDtypeStruct((PB, WIDE), jnp.float32), square, square, square),
        in_specs=[VMEM, VMEM],
        out_specs=(VMEM, VMEM, VMEM, VMEM),
        scratch_shapes=scratch,
        compiler_params=pltpu.CompilerParams(
            collective_id=0, has_side_effects=True, vmem_limit_bytes=40 * 2**20
        ),
        cost_estimate=pl.CostEstimate(flops=600_000_000, bytes_accessed=6_000_000, transcendentals=600),
        name="reduce",
    )(panel, trailing)


def update_kernel(panel, inverse, sums, trailing, factor, factor_next, projection, updated, upper, upper_next, basis):
    at = pl.program_id(0) * TILE

    @pl.when(pl.program_id(0) == 0)
    def _():
        basis[...] = dot(panel[...], inverse[...], (1, 1))
        upper[...] = factor[...]
        upper_next[...] = factor_next[...]

    coefficients = dot(inverse[...], sums[:, pl.ds(aligned(CROSS + at, PB), TILE)] * INV_ROWS)
    projection[...] = coefficients
    updated[...] = trailing[:, pl.ds(aligned(at, PB), TILE)] - dot(basis[...], coefficients)


TILE = 512


def update(panel, inverse, sums, trailing, factor, factor_next):
    wide = jax.ShapeDtypeStruct((PB, TC), jnp.float32)
    square = jax.ShapeDtypeStruct((PB, PB), jnp.float32)
    whole = pl.BlockSpec((PB, PB), lambda i: (0, 0))
    tile = pl.BlockSpec((PB, TILE), lambda i: (0, i))
    return pl.pallas_call(
        update_kernel,
        out_shape=(wide, wide, square, square),
        grid=(TC // TILE,),
        in_specs=[VMEM] * 6,
        out_specs=(tile, tile, whole, whole),
        scratch_shapes=[pltpu.VMEM((PB, PB), jnp.float32)],
        compiler_params=pltpu.CompilerParams(vmem_limit_bytes=24 * 2**20),
        cost_estimate=pl.CostEstimate(flops=600_000_000, bytes_accessed=9_000_000, transcendentals=0),
        name="update",
    )(panel, inverse, sums, trailing, factor, factor_next)


def per_device(panel, trailing):
    sums, factor, inverse, factor_next = reduced(panel, trailing)
    projection, updated, upper_panel, upper_next = update(panel, inverse, sums, trailing, factor, factor_next)
    return (upper_panel, projection, updated, upper_next)


def solution(mesh):
    return jax.shard_map(
        per_device,
        mesh=mesh,
        in_specs=(P(("rows", "grp"), None), P(("rows", "grp"), None)),
        out_specs=(P(), P(), P(("rows", "grp"), None), P()),
        check_vma=False,
    )
```

```python
import jax
import jax.numpy as jnp
from jax import lax
from jax.experimental import pallas as pl
from jax.experimental.pallas import tpu as pltpu
from jax.sharding import PartitionSpec as P

PB = 256
TC = 2048
WIDE = TC + 2 * PB
HALF = 128
SUB = 8
NX, NY, NZ = 4, 4, 8
INV_ROWS = 1.0 / 65536
VMEM = pl.BlockSpec(memory_space=pltpu.VMEM)


def dot(left, right, dims=(1, 0)):
    return lax.dot_general(
        left,
        right,
        (((dims[0],), (dims[1],)), ((), ())),
        precision=lax.Precision.HIGHEST,
        preferred_element_type=jnp.float32,
    )


def identity(order):
    rows = lax.broadcasted_iota(jnp.int32, (order, order), 0)
    columns = lax.broadcasted_iota(jnp.int32, (order, order), 1)
    return (rows == columns).astype(jnp.float32)


def aligned(value, step):
    return pl.multiple_of(value, step)


class Stream:
    def __init__(self, place, acc, out, first, width, x_first, split_z, bufs, send, recv):
        self.acc, self.out = acc, out
        self.columns = pl.ds(first, width)
        self.first, self.width, self.split_z = first, width, split_z
        self.core_buf, self.major_buf, self.minor_buf, self.z_buf = bufs
        self.send, self.recv = send, recv
        self.place = place
        x, y, z, core = place
        self.x_first = x_first
        self.major, self.minor = (x, y) if x_first else (y, x)
        self.base = core * 128
        self.slab = self.base + self.major * 32
        self.own = self.slab + self.minor * 8

    def device(self, axis, value):
        x, y, z, core = self.place
        if axis == "major":
            axis = "x" if self.x_first else "y"
        elif axis == "minor":
            axis = "y" if self.x_first else "x"
        if axis == "x":
            x = value
        elif axis == "y":
            y = value
        elif axis == "z":
            z = value
        else:
            core = value
        return ((y * NZ + z) * 2 + core, x)

    def rows(self, start, size):
        return pl.ds(aligned(start, 8), size)

    def piece(self, z):
        part = self.width // NZ
        return pl.ds(aligned(self.first + z * part, 128), part)

    def phase(self, name):
        acc, out, columns, z = self.acc, self.out, self.columns, self.place[2]
        other = 1 - self.place[3]
        if name == "core":
            return [(acc.at[self.rows(other * 128, 128), columns], self.core_buf, "core", other)]
        if name == "core_share":
            here = out.at[self.rows(self.base, 128), columns]
            return [(here, here, "core", other)]
        copies = []
        for d in range(1, NZ if name in ("z", "z_share") else 4):
            if name == "major":
                peer = lax.rem(self.major + d, 4)
                src = acc.at[self.rows(self.base + peer * 32, 32), columns]
                copies.append((src, self.major_buf.at[d - 1], "major", peer))
            elif name == "minor":
                peer = lax.rem(self.minor + d, 4)
                src = acc.at[self.rows(self.slab + peer * 8, 8), columns]
                copies.append((src, self.minor_buf.at[d - 1], "minor", peer))
            elif name == "z":
                peer = lax.rem(z + d, NZ)
                src = acc.at[self.rows(self.own, 8), self.piece(peer) if self.split_z else columns]
                copies.append((src, self.z_buf.at[d - 1], "z", peer))
            elif name == "z_share":
                here = out.at[self.rows(self.own, 8), self.piece(z)]
                copies.append((here, here, "z", lax.rem(z + d, NZ)))
            elif name == "minor_share":
                here = out.at[self.rows(self.own, 8), columns]
                copies.append((here, here, "minor", lax.rem(self.minor + d, 4)))
            else:
                here = out.at[self.rows(self.slab, 32), columns]
                copies.append((here, here, "major", lax.rem(self.major + d, 4)))
        return copies

    def copies(self, name):
        return [
            pltpu.make_async_remote_copy(
                src_ref=src,
                dst_ref=dst,
                send_sem=self.send.at[FIRST[name] + index],
                recv_sem=self.recv.at[FIRST[name] + index],
                device_id=self.device(axis, peer),
                device_id_type=pl.DeviceIdType.MESH,
            )
            for index, (src, dst, axis, peer) in enumerate(self.phase(name))
        ]

    def start(self, name):
        if name == "z_share" and not self.split_z:
            return
        for copy in self.copies(name):
            copy.start()

    def wait(self, name):
        if name == "z_share" and not self.split_z:
            return
        for copy in self.copies(name):
            copy.wait()

    def core_end(self):
        self.wait("core")

        @pl.loop(0, 16)
        def _(step):
            here = self.rows(self.base + step * 8, 8)
            there = pl.ds(aligned(step * 8, 8), 8)
            self.acc[here, self.columns] = self.acc[here, self.columns] + self.core_buf[there, :]

    def major_end(self):
        self.wait("major")

        @pl.loop(0, 4)
        def _(step):
            here = self.rows(self.slab + step * 8, 8)
            there = pl.ds(aligned(step * 8, 8), 8)
            total = self.acc[here, self.columns]
            for d in range(3):
                total = total + self.major_buf[d, there, :]
            self.acc[here, self.columns] = total

    def minor_end(self):
        self.wait("minor")
        here = self.rows(self.own, 8)
        total = self.acc[here, self.columns]
        for d in range(3):
            total = total + self.minor_buf[d]
        self.acc[here, self.columns] = total

    def z_end(self):
        self.wait("z")
        here = self.rows(self.own, 8)
        columns = self.piece(self.place[2]) if self.split_z else self.columns
        total = self.acc[here, columns]
        for d in range(NZ - 1):
            total = total + self.z_buf[d]
        self.out[here, columns] = total

    def turn(self, before, after):
        self.wait(before)
        self.start(after)


FIRST = {
    "core": 0,
    "major": 1,
    "minor": 4,
    "z": 7,
    "z_share": 14,
    "minor_share": 21,
    "major_share": 24,
    "core_share": 27,
}
COPIES = 28

CROSS = 2 * PB
STREAMS = ((0, 256, True, False), (256, 512, False, False), (768, 1024, True, True), (1792, 768, False, False))


def greet(place):
    x, y, z, core = place
    peers = [((y * NZ + z) * 2 + 1 - core, x)]
    peers += [((y * NZ + z) * 2 + core, lax.rem(x + d, NX)) for d in range(1, NX)]
    peers += [((lax.rem(y + d, NY) * NZ + z) * 2 + core, x) for d in range(1, NY)]
    peers += [((y * NZ + lax.rem(z + d, NZ)) * 2 + core, x) for d in range(1, NZ)]
    barrier = pltpu.get_barrier_semaphore()
    for peer in peers:
        pl.semaphore_signal(barrier, inc=1, device_id=peer, device_id_type=pl.DeviceIdType.MESH)
    return barrier, len(peers)


def factor_half(work, upper, inverse, between):
    full = (SUB, HALF)
    lane = lax.broadcasted_iota(jnp.int32, (1, HALF), 1)
    for block in range(HALF // SUB):
        between(block)
        base = block * SUB
        left = [jnp.broadcast_to(work[base + i : base + i + 1, :HALF], full) for i in range(SUB)]
        right = [jnp.broadcast_to(work[base + i : base + i + 1, HALF:], full) for i in range(SUB)]
        entry = [
            [jnp.broadcast_to(left[i][:, base + k : base + k + 1], full) for k in range(i + 1)]
            for i in range(SUB)
        ]
        unit = [[None] * SUB for _ in range(SUB)]
        recip = [None] * SUB
        for k in range(SUB):
            recip[k] = 1.0 / entry[k][k]
            for j in range(k + 1, SUB):
                unit[j][k] = entry[j][k] * recip[k]
            for j in range(k + 1, SUB):
                for i in range(j, SUB):
                    entry[i][j] = entry[i][j] - entry[i][k] * unit[j][k]
                left[j] = left[j] - unit[j][k] * left[k]
                right[j] = right[j] - unit[j][k] * right[k]
        for k in range(SUB):
            scale = lax.rsqrt(entry[k][k])
            row = base + k
            upper[row : row + 1, :] = jnp.where(lane >= row, (left[k] * scale)[0:1, :], 0.0)
            inverse[row : row + 1, :] = (right[k] * scale)[0:1, :]
        if base + SUB == HALF:
            break
        for k in range(SUB - 1, -1, -1):
            left[k] = left[k] * recip[k]
            right[k] = right[k] * recip[k]
            for j in range(k + 1, SUB):
                left[k] = left[k] - unit[j][k] * left[j]
                right[k] = right[k] - unit[j][k] * right[j]
        for other in range(base + SUB, HALF, SUB):
            rows = slice(other, other + SUB)
            lead = work[rows, :HALF]
            tail = work[rows, HALF:]
            column = [jnp.broadcast_to(lead[:, base + k : base + k + 1], full) for k in range(SUB)]
            for k in range(SUB):
                lead = lead - column[k] * left[k]
                tail = tail - column[k] * right[k]
            work[rows, :HALF] = lead
            work[rows, HALF:] = tail


def reduce_kernel(panel, trailing, out, upper, inverse, upper_next, acc, work, halves, inverses, middle, schur, *scratch):
    row = lax.axis_index("rows")
    x = lax.axis_index("grp")
    core = lax.rem(row, 2)
    z = lax.rem(row // 2, NZ)
    y = row // (2 * NZ)
    place = (x, y, z, core)
    barrier, greeted = greet(place)

    streams = []
    for index, (first, width, x_first, split_z) in enumerate(STREAMS):
        bufs, send, recv = scratch[6 * index : 6 * index + 4], *scratch[6 * index + 4 : 6 * index + 6]
        streams.append(Stream(place, acc, out, first, width, x_first, split_z, bufs, send, recv))
    gram, head, one, two = streams

    def products(first, last):
        @pl.loop(first, last)
        def _(tile):
            columns = pl.ds(aligned(tile * PB, PB), PB)
            acc[:, pl.ds(aligned(CROSS + tile * PB, PB), PB)] = dot(panel[...], trailing[:, columns], (0, 0))

    acc[:, :PB] = dot(panel[...], panel[...], (0, 0))
    pl.semaphore_wait(barrier, greeted)
    gram.start("core")
    acc[:, PB : 2 * PB] = dot(trailing[:, :PB], trailing[:, :PB], (0, 0))
    acc[:, CROSS : CROSS + PB] = dot(panel[...], trailing[:, :PB], (0, 0))
    gram.core_end()
    gram.start("major")
    head.start("core")
    products(1, 5)
    one.start("core")
    head.core_end()
    head.start("major")
    gram.major_end()
    gram.start("minor")
    one.core_end()
    one.start("major")
    products(5, TC // PB)
    two.start("core")
    gram.minor_end()
    gram.start("z")
    two.core_end()
    two.start("major")
    head.major_end()
    head.start("minor")
    gram.z_end()
    gram.start("minor_share")
    head.minor_end()
    head.start("z")
    one.major_end()
    one.start("minor")
    two.major_end()
    two.start("minor")
    gram.turn("minor_share", "major_share")
    one.minor_end()
    one.start("z")
    two.minor_end()
    two.start("z")
    gram.turn("major_share", "core_share")
    head.z_end()
    head.start("minor_share")
    gram.wait("core_share")

    def meet_first():
        one.z_end()
        one.start("z_share")

    def meet_second():
        head.turn("minor_share", "major_share")

    def meet_third():
        two.z_end()
        two.start("minor_share")
        one.turn("z_share", "minor_share")

    def meet_fourth():
        head.turn("major_share", "core_share")

    def meet_fifth():
        two.turn("minor_share", "major_share")

    def meet_sixth():
        one.turn("minor_share", "major_share")
        head.wait("core_share")

    def meet_seventh():
        two.turn("major_share", "core_share")

    def meet_last():
        one.turn("major_share", "core_share")

    meetings = (
        (0, 3, meet_first),
        (0, 6, meet_second),
        (1, 2, meet_third),
        (1, 7, meet_fourth),
        (1, 12, meet_fifth),
        (1, 15, meet_sixth),
        (3, 2, meet_seventh),
        (3, 9, meet_last),
    )

    zeros = jnp.zeros((HALF, HALF), jnp.float32)
    work[:, :HALF] = out[:HALF, :HALF] * INV_ROWS
    work[:, HALF:] = identity(HALF)
    schur[...] = out[:, :PB] * INV_ROWS

    @pl.loop(0, 4)
    def _(step):
        @pl.when(lax.rem(step, 2) == 1)
        def _():
            cross = dot(inverses[0], schur[:HALF, HALF:])
            middle[...] = cross
            work[:, :HALF] = schur[HALF:, HALF:] - dot(cross, cross, (0, 0))
            work[:, HALF:] = identity(HALF)

        @pl.when(step == 2)
        def _():
            upper[:HALF, :HALF] = halves[0]
            upper[:HALF, HALF:] = middle[...]
            upper[HALF:, :HALF] = zeros
            upper[HALF:, HALF:] = halves[1]
            inverse[:HALF, :HALF] = inverses[0]
            inverse[:HALF, HALF:] = zeros
            inverse[HALF:, :HALF] = -dot(inverses[1], dot(middle[...], inverses[0], (0, 0)))
            inverse[HALF:, HALF:] = inverses[1]
            part = dot(inverse[...], out[:, CROSS : CROSS + PB] * INV_ROWS)
            schur[...] = out[:, PB : 2 * PB] * INV_ROWS - dot(part, part, (0, 0))
            work[:, :HALF] = schur[:HALF, :HALF]
            work[:, HALF:] = identity(HALF)

        def between(block):
            for at_step, at_block, action in meetings:
                if at_block == block:
                    pl.when(step == at_step)(action)

        at = lax.rem(step, 2)
        factor_half(work, halves.at[at], inverses.at[at], between)

    upper_next[:HALF, :HALF] = halves[0]
    upper_next[:HALF, HALF:] = middle[...]
    upper_next[HALF:, :HALF] = zeros
    upper_next[HALF:, HALF:] = halves[1]
    one.wait("core_share")
    two.wait("core_share")


def reduced(panel, trailing):
    square = jax.ShapeDtypeStruct((PB, PB), jnp.float32)
    scratch = [
        pltpu.VMEM((PB, WIDE), jnp.float32),
        pltpu.VMEM((HALF, PB), jnp.float32),
        pltpu.VMEM((2, HALF, HALF), jnp.float32),
        pltpu.VMEM((2, HALF, HALF), jnp.float32),
        pltpu.VMEM((HALF, HALF), jnp.float32),
        pltpu.VMEM((PB, PB), jnp.float32),
    ]
    for _, width, _, split_z in STREAMS:
        part = width // NZ if split_z else width
        scratch += [
            pltpu.VMEM((128, width), jnp.float32),
            pltpu.VMEM((3, 32, width), jnp.float32),
            pltpu.VMEM((3, 8, width), jnp.float32),
            pltpu.VMEM((NZ - 1, 8, part), jnp.float32),
            pltpu.SemaphoreType.DMA((COPIES,)),
            pltpu.SemaphoreType.DMA((COPIES,)),
        ]
    return pl.pallas_call(
        reduce_kernel,
        out_shape=(jax.ShapeDtypeStruct((PB, WIDE), jnp.float32), square, square, square),
        in_specs=[VMEM, VMEM],
        out_specs=(VMEM, VMEM, VMEM, VMEM),
        scratch_shapes=scratch,
        compiler_params=pltpu.CompilerParams(
            collective_id=0, has_side_effects=True, vmem_limit_bytes=40 * 2**20
        ),
        cost_estimate=pl.CostEstimate(flops=600_000_000, bytes_accessed=6_000_000, transcendentals=600),
        name="reduce",
    )(panel, trailing)


def update_kernel(panel, inverse, sums, trailing, factor, factor_next, projection, updated, upper, upper_next, basis):
    at = pl.program_id(0) * TILE

    @pl.when(pl.program_id(0) == 0)
    def _():
        basis[...] = dot(panel[...], inverse[...], (1, 1))
        upper[...] = factor[...]
        upper_next[...] = factor_next[...]

    coefficients = dot(inverse[...], sums[:, pl.ds(aligned(CROSS + at, PB), TILE)] * INV_ROWS)
    projection[...] = coefficients
    updated[...] = trailing[:, pl.ds(aligned(at, PB), TILE)] - dot(basis[...], coefficients)


TILE = 512


def update(panel, inverse, sums, trailing, factor, factor_next):
    wide = jax.ShapeDtypeStruct((PB, TC), jnp.float32)
    square = jax.ShapeDtypeStruct((PB, PB), jnp.float32)
    whole = pl.BlockSpec((PB, PB), lambda i: (0, 0))
    tile = pl.BlockSpec((PB, TILE), lambda i: (0, i))
    return pl.pallas_call(
        update_kernel,
        out_shape=(wide, wide, square, square),
        grid=(TC // TILE,),
        in_specs=[VMEM] * 6,
        out_specs=(tile, tile, whole, whole),
        scratch_shapes=[pltpu.VMEM((PB, PB), jnp.float32)],
        compiler_params=pltpu.CompilerParams(vmem_limit_bytes=24 * 2**20),
        cost_estimate=pl.CostEstimate(flops=600_000_000, bytes_accessed=9_000_000, transcendentals=0),
        name="update",
    )(panel, inverse, sums, trailing, factor, factor_next)


def per_device(panel, trailing):
    sums, factor, inverse, factor_next = reduced(panel, trailing)
    projection, updated, upper_panel, upper_next = update(panel, inverse, sums, trailing, factor, factor_next)
    return (upper_panel, projection, updated, upper_next)


def solution(mesh):
    return jax.shard_map(
        per_device,
        mesh=mesh,
        in_specs=(P(("rows", "grp"), None), P(("rows", "grp"), None)),
        out_specs=(P(), P(), P(("rows", "grp"), None), P()),
        check_vma=False,
    )
```

```python
import jax
import jax.numpy as jnp
from jax import lax
from jax.experimental import pallas as pl
from jax.experimental.pallas import tpu as pltpu
from jax.sharding import PartitionSpec as P

PB = 256
TC = 2048
WIDE = TC + 2 * PB
HALF = 128
SUB = 8
NX, NY, NZ = 4, 4, 8
INV_ROWS = 1.0 / 65536
VMEM = pl.BlockSpec(memory_space=pltpu.VMEM)


def dot(left, right, dims=(1, 0)):
    return lax.dot_general(
        left,
        right,
        (((dims[0],), (dims[1],)), ((), ())),
        precision=lax.Precision.HIGHEST,
        preferred_element_type=jnp.float32,
    )


def identity(order):
    rows = lax.broadcasted_iota(jnp.int32, (order, order), 0)
    columns = lax.broadcasted_iota(jnp.int32, (order, order), 1)
    return (rows == columns).astype(jnp.float32)


def aligned(value, step):
    return pl.multiple_of(value, step)


class Stream:
    def __init__(self, place, acc, out, first, width, x_first, split_z, bufs, send, recv):
        self.acc, self.out = acc, out
        self.columns = pl.ds(first, width)
        self.first, self.width, self.split_z = first, width, split_z
        self.core_buf, self.major_buf, self.minor_buf, self.z_buf = bufs
        self.send, self.recv = send, recv
        self.place = place
        x, y, z, core = place
        self.x_first = x_first
        self.major, self.minor = (x, y) if x_first else (y, x)
        self.base = core * 128
        self.slab = self.base + self.major * 32
        self.own = self.slab + self.minor * 8

    def device(self, axis, value):
        x, y, z, core = self.place
        if axis == "major":
            axis = "x" if self.x_first else "y"
        elif axis == "minor":
            axis = "y" if self.x_first else "x"
        if axis == "x":
            x = value
        elif axis == "y":
            y = value
        elif axis == "z":
            z = value
        else:
            core = value
        return ((y * NZ + z) * 2 + core, x)

    def rows(self, start, size):
        return pl.ds(aligned(start, 8), size)

    def piece(self, z):
        part = self.width // NZ
        return pl.ds(aligned(self.first + z * part, 128), part)

    def phase(self, name):
        acc, out, columns, z = self.acc, self.out, self.columns, self.place[2]
        other = 1 - self.place[3]
        if name == "core":
            return [(acc.at[self.rows(other * 128, 128), columns], self.core_buf, "core", other)]
        if name == "core_share":
            here = out.at[self.rows(self.base, 128), columns]
            return [(here, here, "core", other)]
        copies = []
        for d in range(1, NZ if name in ("z", "z_share") else 4):
            if name == "major":
                peer = lax.rem(self.major + d, 4)
                src = acc.at[self.rows(self.base + peer * 32, 32), columns]
                copies.append((src, self.major_buf.at[d - 1], "major", peer))
            elif name == "minor":
                peer = lax.rem(self.minor + d, 4)
                src = acc.at[self.rows(self.slab + peer * 8, 8), columns]
                copies.append((src, self.minor_buf.at[d - 1], "minor", peer))
            elif name == "z":
                peer = lax.rem(z + d, NZ)
                src = acc.at[self.rows(self.own, 8), self.piece(peer) if self.split_z else columns]
                copies.append((src, self.z_buf.at[d - 1], "z", peer))
            elif name == "z_share":
                here = out.at[self.rows(self.own, 8), self.piece(z)]
                copies.append((here, here, "z", lax.rem(z + d, NZ)))
            elif name == "minor_share":
                here = out.at[self.rows(self.own, 8), columns]
                copies.append((here, here, "minor", lax.rem(self.minor + d, 4)))
            else:
                here = out.at[self.rows(self.slab, 32), columns]
                copies.append((here, here, "major", lax.rem(self.major + d, 4)))
        return copies

    def copies(self, name):
        return [
            pltpu.make_async_remote_copy(
                src_ref=src,
                dst_ref=dst,
                send_sem=self.send.at[FIRST[name] + index],
                recv_sem=self.recv.at[FIRST[name] + index],
                device_id=self.device(axis, peer),
                device_id_type=pl.DeviceIdType.MESH,
            )
            for index, (src, dst, axis, peer) in enumerate(self.phase(name))
        ]

    def start(self, name):
        if name == "z_share" and not self.split_z:
            return
        for copy in self.copies(name):
            copy.start()

    def wait(self, name):
        if name == "z_share" and not self.split_z:
            return
        for copy in self.copies(name):
            copy.wait()

    def core_end(self):
        self.wait("core")

        @pl.loop(0, 16)
        def _(step):
            here = self.rows(self.base + step * 8, 8)
            there = pl.ds(aligned(step * 8, 8), 8)
            self.acc[here, self.columns] = self.acc[here, self.columns] + self.core_buf[there, :]

    def major_end(self):
        self.wait("major")

        @pl.loop(0, 4)
        def _(step):
            here = self.rows(self.slab + step * 8, 8)
            there = pl.ds(aligned(step * 8, 8), 8)
            total = self.acc[here, self.columns]
            for d in range(3):
                total = total + self.major_buf[d, there, :]
            self.acc[here, self.columns] = total

    def minor_end(self):
        self.wait("minor")
        here = self.rows(self.own, 8)
        total = self.acc[here, self.columns]
        for d in range(3):
            total = total + self.minor_buf[d]
        self.acc[here, self.columns] = total

    def z_end(self):
        self.wait("z")
        here = self.rows(self.own, 8)
        columns = self.piece(self.place[2]) if self.split_z else self.columns
        total = self.acc[here, columns]
        for d in range(NZ - 1):
            total = total + self.z_buf[d]
        self.out[here, columns] = total

    def turn(self, before, after):
        self.wait(before)
        self.start(after)


FIRST = {
    "core": 0,
    "major": 1,
    "minor": 4,
    "z": 7,
    "z_share": 14,
    "minor_share": 21,
    "major_share": 24,
    "core_share": 27,
}
COPIES = 28

CROSS = 2 * PB
STREAMS = ((0, 256, True, False), (256, 512, False, False), (768, 1024, True, True), (1792, 768, False, False))


def greet(place):
    x, y, z, core = place
    peers = [((y * NZ + z) * 2 + 1 - core, x)]
    peers += [((y * NZ + z) * 2 + core, lax.rem(x + d, NX)) for d in range(1, NX)]
    peers += [((lax.rem(y + d, NY) * NZ + z) * 2 + core, x) for d in range(1, NY)]
    peers += [((y * NZ + lax.rem(z + d, NZ)) * 2 + core, x) for d in range(1, NZ)]
    barrier = pltpu.get_barrier_semaphore()
    for peer in peers:
        pl.semaphore_signal(barrier, inc=1, device_id=peer, device_id_type=pl.DeviceIdType.MESH)
    return barrier, len(peers)


def factor_half(work, upper, inverse, between, inverted):
    full = (SUB, HALF)
    lane = lax.broadcasted_iota(jnp.int32, (1, HALF), 1)
    for block in range(HALF // SUB):
        between(block)
        base = block * SUB
        left = [jnp.broadcast_to(work[base + i : base + i + 1, :HALF], full) for i in range(SUB)]
        right = [jnp.broadcast_to(work[base + i : base + i + 1, HALF:], full) for i in range(SUB)]
        entry = [
            [jnp.broadcast_to(left[i][:, base + k : base + k + 1], full) for k in range(i + 1)]
            for i in range(SUB)
        ]
        unit = [[None] * SUB for _ in range(SUB)]
        recip = [None] * SUB
        for k in range(SUB):
            recip[k] = 1.0 / entry[k][k]
            for j in range(k + 1, SUB):
                unit[j][k] = entry[j][k] * recip[k]
            for j in range(k + 1, SUB):
                for i in range(j, SUB):
                    entry[i][j] = entry[i][j] - entry[i][k] * unit[j][k]
                left[j] = left[j] - unit[j][k] * left[k]
                if inverted:
                    right[j] = right[j] - unit[j][k] * right[k]
        for k in range(SUB):
            scale = lax.rsqrt(entry[k][k])
            row = base + k
            upper[row : row + 1, :] = jnp.where(lane >= row, (left[k] * scale)[0:1, :], 0.0)
            if inverted:
                inverse[row : row + 1, :] = (right[k] * scale)[0:1, :]
        if base + SUB == HALF:
            break
        for k in range(SUB - 1, -1, -1):
            left[k] = left[k] * recip[k]
            for j in range(k + 1, SUB):
                left[k] = left[k] - unit[j][k] * left[j]
            if inverted:
                right[k] = right[k] * recip[k]
                for j in range(k + 1, SUB):
                    right[k] = right[k] - unit[j][k] * right[j]
        for other in range(base + SUB, HALF, SUB):
            rows = slice(other, other + SUB)
            lead = work[rows, :HALF]
            tail = work[rows, HALF:]
            column = [jnp.broadcast_to(lead[:, base + k : base + k + 1], full) for k in range(SUB)]
            for k in range(SUB):
                lead = lead - column[k] * left[k]
                if inverted:
                    tail = tail - column[k] * right[k]
            work[rows, :HALF] = lead
            if inverted:
                work[rows, HALF:] = tail


def reduce_kernel(
    panel_hbm,
    trailing_hbm,
    out,
    upper,
    inverse,
    upper_next,
    basis,
    panel,
    trailing,
    load,
    acc,
    work,
    halves,
    inverses,
    middle,
    schur,
    *scratch,
):
    row = lax.axis_index("rows")
    x = lax.axis_index("grp")
    core = lax.rem(row, 2)
    z = lax.rem(row // 2, NZ)
    y = row // (2 * NZ)
    place = (x, y, z, core)
    loads = [
        pltpu.make_async_copy(panel_hbm, panel, load.at[0]),
        pltpu.make_async_copy(trailing_hbm, trailing, load.at[1]),
    ]
    for copy in loads:
        copy.start()
    barrier, greeted = greet(place)

    streams = []
    for index, (first, width, x_first, split_z) in enumerate(STREAMS):
        bufs, send, recv = scratch[6 * index : 6 * index + 4], *scratch[6 * index + 4 : 6 * index + 6]
        streams.append(Stream(place, acc, out, first, width, x_first, split_z, bufs, send, recv))
    gram, head, one, two = streams

    def products(first, last):
        @pl.loop(first, last)
        def _(tile):
            columns = pl.ds(aligned(tile * PB, PB), PB)
            acc[:, pl.ds(aligned(CROSS + tile * PB, PB), PB)] = dot(panel[...], trailing[:, columns], (0, 0))

    loads[0].wait()
    acc[:, :PB] = dot(panel[...], panel[...], (0, 0))
    loads[1].wait()
    pl.semaphore_wait(barrier, greeted)
    gram.start("core")
    acc[:, PB : 2 * PB] = dot(trailing[:, :PB], trailing[:, :PB], (0, 0))
    acc[:, CROSS : CROSS + PB] = dot(panel[...], trailing[:, :PB], (0, 0))
    gram.core_end()
    gram.start("major")
    head.start("core")
    products(1, 5)
    one.start("core")
    head.core_end()
    head.start("major")
    gram.major_end()
    gram.start("minor")
    one.core_end()
    one.start("major")
    products(5, TC // PB)
    two.start("core")
    gram.minor_end()
    gram.start("z")
    two.core_end()
    two.start("major")
    head.major_end()
    head.start("minor")
    gram.z_end()
    gram.start("minor_share")
    head.minor_end()
    head.start("z")
    one.major_end()
    one.start("minor")
    two.major_end()
    two.start("minor")
    gram.turn("minor_share", "major_share")
    one.minor_end()
    one.start("z")
    two.minor_end()
    two.start("z")
    gram.turn("major_share", "core_share")
    head.z_end()
    head.start("minor_share")
    gram.wait("core_share")

    def meet_first():
        one.z_end()
        one.start("z_share")

    def meet_second():
        head.turn("minor_share", "major_share")

    def meet_third():
        two.z_end()
        two.start("minor_share")
        one.turn("z_share", "minor_share")

    def meet_fourth():
        head.turn("major_share", "core_share")

    def meet_fifth():
        two.turn("minor_share", "major_share")

    def meet_sixth():
        one.turn("minor_share", "major_share")
        head.wait("core_share")

    def meet_seventh():
        two.turn("major_share", "core_share")

    def meet_last():
        one.turn("major_share", "core_share")

    meetings = (
        (0, 3, meet_first),
        (0, 6, meet_second),
        (1, 2, meet_third),
        (1, 7, meet_fourth),
        (1, 12, meet_fifth),
        (1, 15, meet_sixth),
        (3, 2, meet_seventh),
        (3, 9, meet_last),
    )

    zeros = jnp.zeros((HALF, HALF), jnp.float32)
    work[:, :HALF] = out[:HALF, :HALF] * INV_ROWS
    work[:, HALF:] = identity(HALF)
    schur[...] = out[:, :PB] * INV_ROWS

    for step in range(4):
        if step % 2 == 1:
            cross = dot(inverses[0], schur[:HALF, HALF:])
            middle[...] = cross
            work[:, :HALF] = schur[HALF:, HALF:] - dot(cross, cross, (0, 0))
            work[:, HALF:] = identity(HALF)
        if step == 2:
            upper[:HALF, :HALF] = halves[0]
            upper[:HALF, HALF:] = middle[...]
            upper[HALF:, :HALF] = zeros
            upper[HALF:, HALF:] = halves[1]
            inverse[:HALF, :HALF] = inverses[0]
            inverse[:HALF, HALF:] = zeros
            inverse[HALF:, :HALF] = -dot(inverses[1], dot(middle[...], inverses[0], (0, 0)))
            inverse[HALF:, HALF:] = inverses[1]
            part = dot(inverse[...], out[:, CROSS : CROSS + PB] * INV_ROWS)
            schur[...] = out[:, PB : 2 * PB] * INV_ROWS - dot(part, part, (0, 0))
            work[:, :HALF] = schur[:HALF, :HALF]
            work[:, HALF:] = identity(HALF)

        def between(block):
            for at_step, at_block, action in meetings:
                if at_step == step and at_block == block:
                    action()

        factor_half(work, halves.at[step % 2], inverses.at[step % 2], between, step < 3)

    upper_next[:HALF, :HALF] = halves[0]
    upper_next[:HALF, HALF:] = middle[...]
    upper_next[HALF:, :HALF] = zeros
    upper_next[HALF:, HALF:] = halves[1]
    basis[...] = dot(panel[...], inverse[...], (1, 1))
    two.wait("core_share")
    one.wait("core_share")


def reduced(panel, trailing):
    square = jax.ShapeDtypeStruct((PB, PB), jnp.float32)
    scratch = [
        pltpu.VMEM((PB, PB), jnp.float32),
        pltpu.VMEM((PB, TC), jnp.float32),
        pltpu.SemaphoreType.DMA((2,)),
        pltpu.VMEM((PB, WIDE), jnp.float32),
        pltpu.VMEM((HALF, PB), jnp.float32),
        pltpu.VMEM((2, HALF, HALF), jnp.float32),
        pltpu.VMEM((2, HALF, HALF), jnp.float32),
        pltpu.VMEM((HALF, HALF), jnp.float32),
        pltpu.VMEM((PB, PB), jnp.float32),
    ]
    for _, width, _, split_z in STREAMS:
        part = width // NZ if split_z else width
        scratch += [
            pltpu.VMEM((128, width), jnp.float32),
            pltpu.VMEM((3, 32, width), jnp.float32),
            pltpu.VMEM((3, 8, width), jnp.float32),
            pltpu.VMEM((NZ - 1, 8, part), jnp.float32),
            pltpu.SemaphoreType.DMA((COPIES,)),
            pltpu.SemaphoreType.DMA((COPIES,)),
        ]
    return pl.pallas_call(
        reduce_kernel,
        out_shape=(jax.ShapeDtypeStruct((PB, WIDE), jnp.float32), square, square, square, square),
        in_specs=[pl.BlockSpec(memory_space=pltpu.HBM)] * 2,
        out_specs=(VMEM, VMEM, VMEM, VMEM, VMEM),
        scratch_shapes=scratch,
        compiler_params=pltpu.CompilerParams(
            collective_id=0, has_side_effects=True, vmem_limit_bytes=40 * 2**20
        ),
        cost_estimate=pl.CostEstimate(flops=600_000_000, bytes_accessed=6_000_000, transcendentals=600),
        name="reduce",
    )(panel, trailing)


def halves_of(value):
    high = value.astype(jnp.bfloat16)
    return high, (value - high.astype(jnp.float32)).astype(jnp.bfloat16)


def product(left, right):
    return jnp.dot(left, right, preferred_element_type=jnp.float32)


def update_kernel(basis, inverse, sums, trailing, factor, factor_next, projection, updated, upper, upper_next, coarse, fine):
    at = pl.program_id(0) * TILE

    @pl.when(pl.program_id(0) == 0)
    def _():
        upper[...] = factor[...]
        upper_next[...] = factor_next[...]
        coarse[...], fine[...] = halves_of(basis[...])

    coefficients = dot(inverse[...], sums[:, pl.ds(aligned(CROSS + at, PB), TILE)] * INV_ROWS)
    projection[...] = coefficients
    high, low = halves_of(coefficients)
    span = product(coarse[...], high) + (product(coarse[...], low) + product(fine[...], high))
    updated[...] = trailing[:, pl.ds(aligned(at, PB), TILE)] - span


TILE = 512


def update(basis, inverse, sums, trailing, factor, factor_next):
    wide = jax.ShapeDtypeStruct((PB, TC), jnp.float32)
    square = jax.ShapeDtypeStruct((PB, PB), jnp.float32)
    whole = pl.BlockSpec((PB, PB), lambda i: (0, 0))
    tile = pl.BlockSpec((PB, TILE), lambda i: (0, i))
    return pl.pallas_call(
        update_kernel,
        out_shape=(wide, wide, square, square),
        grid=(TC // TILE,),
        in_specs=[VMEM] * 6,
        out_specs=(tile, tile, whole, whole),
        scratch_shapes=[pltpu.VMEM((PB, PB), jnp.bfloat16)] * 2,
        compiler_params=pltpu.CompilerParams(vmem_limit_bytes=24 * 2**20),
        cost_estimate=pl.CostEstimate(flops=600_000_000, bytes_accessed=9_000_000, transcendentals=0),
        name="update",
    )(basis, inverse, sums, trailing, factor, factor_next)


def per_device(panel, trailing):
    sums, factor, inverse, factor_next, basis = reduced(panel, trailing)
    projection, updated, upper_panel, upper_next = update(basis, inverse, sums, trailing, factor, factor_next)
    return (upper_panel, projection, updated, upper_next)


def solution(mesh):
    return jax.shard_map(
        per_device,
        mesh=mesh,
        in_specs=(P(("rows", "grp"), None), P(("rows", "grp"), None)),
        out_specs=(P(), P(), P(("rows", "grp"), None), P()),
        check_vma=False,
    )
```
